32 devices in a mesh: dp: 2 (over x), tp: 4 (over z), ep: 4 (over y, core).
Axes of the slice: x: 2, y: 2, z: 4, core: 2. Of those that a mesh axis runs over, the one named last changes fastest.
Arguments:
- tokens_x: bfloat16 [2048, 2048], P(('dp', 'ep', 'tp')), parts along dimension 0
- expert_ids: int32 [2048, 6], P(('dp', 'ep', 'tp')), parts along dimension 0
- route_gate: float32 [2048, 6], P(('dp', 'ep', 'tp')), parts along dimension 0
- w_gate: bfloat16 [64, 2048, 1408], P('ep', None, 'tp')
- w_up: bfloat16 [64, 2048, 1408], P('ep', None, 'tp')
- w_down: bfloat16 [64, 1408, 2048], P('ep', 'tp')
Outputs:
- output: bfloat16 [2048, 2048], P(('dp', 'ep', 'tp')), parts along dimension 0
There are 2 independent parts. The reference program is written for one: setup_inputs(seed, part) draws one part's arguments, and reference() takes and returns one part's arrays. A program takes and returns all parts, laid end to end along the dimension named above; an argument that names none is the same for every part.
All inputs are finite; a program needn't handle non-finite values.
Results may differ from the reference program's by a relative error of at most 0.00123.
Values are sent between devices in bfloat16 or wider.
A program may use at most 1 GiB of HBM per device.

```python
import jax
import jax.numpy as jnp
from jax import lax

D_MODEL = 2048
FF_DIM = 1408
EXPERTS = 64
TOP_K = 6
EP_GROUP = 4
TOKENS = 1024


def draw_routing(route_key):
    num_blocks = TOKENS // EXPERTS
    per_dev = EXPERTS // EP_GROUP
    key_pos, key_dev, key_loc = jax.random.split(route_key, 3)
    row_pos = jax.vmap(lambda one_key: jax.random.permutation(one_key, EXPERTS))(jax.random.split(key_pos, num_blocks))
    dev_perm = jax.vmap(lambda one_key: jax.random.permutation(one_key, EP_GROUP))(jax.random.split(key_dev, num_blocks))
    loc_perm = jax.vmap(lambda one_key: jax.random.permutation(one_key, per_dev))(jax.random.split(key_loc, num_blocks * EP_GROUP))
    loc_perm = loc_perm.reshape(num_blocks, EP_GROUP, per_dev)
    slot_offset = jnp.arange(TOP_K, dtype=jnp.int32)

    def block_ids(dev_order, loc_order, positions):
        labels = (positions[:, None] + slot_offset[None, :]) % EXPERTS
        dev_slot = labels % EP_GROUP
        return dev_order[dev_slot] * per_dev + loc_order[dev_slot, labels // EP_GROUP]

    all_ids = jax.vmap(block_ids)(dev_perm, loc_perm, row_pos)
    return all_ids.reshape(TOKENS, TOP_K).astype(jnp.int32)


def setup_inputs(seed: int = 0, part: int = 0) -> dict:
    part_key = jax.random.fold_in(jax.random.key(seed), part)
    key_x, key_gate, key_route = jax.random.split(part_key, 3)
    key_wg, key_wu, key_wd = jax.random.split(jax.random.key(seed + 1), 3)
    tokens_x = jax.random.normal(key_x, (TOKENS, D_MODEL), jnp.float32).astype(jnp.bfloat16)
    expert_ids = draw_routing(key_route)
    route_gate = jax.random.uniform(key_gate, (TOKENS, TOP_K), jnp.float32, 0.5, 1.5) * TOP_K ** -0.5
    w_gate = (jax.random.normal(key_wg, (EXPERTS, D_MODEL, FF_DIM), jnp.float32) * D_MODEL ** -0.5).astype(jnp.bfloat16)
    w_up = (jax.random.normal(key_wu, (EXPERTS, D_MODEL, FF_DIM), jnp.float32) * D_MODEL ** -0.5).astype(jnp.bfloat16)
    w_down = (jax.random.normal(key_wd, (EXPERTS, FF_DIM, D_MODEL), jnp.float32) * FF_DIM ** -0.5).astype(jnp.bfloat16)
    return dict(tokens_x=tokens_x, expert_ids=expert_ids, route_gate=route_gate, w_gate=w_gate, w_up=w_up, w_down=w_down)


def reference(tokens_x, expert_ids, route_gate, w_gate, w_up, w_down):
    expert_cap = TOKENS * TOP_K // EXPERTS
    sort_order = jnp.argsort(expert_ids.reshape(-1), stable=True)
    tok_rows = (sort_order // TOP_K).reshape(EXPERTS, expert_cap)
    gate_rows = route_gate.reshape(-1)[sort_order].reshape(EXPERTS, expert_cap)

    def add_expert(acc_sum, per_expert):
        rows_e, gates_e, wg_e, wu_e, wd_e = per_expert
        x_rows = tokens_x[rows_e]
        h_gate = jnp.dot(x_rows, wg_e, preferred_element_type=jnp.float32)
        h_up = jnp.dot(x_rows, wu_e, preferred_element_type=jnp.float32)
        hidden = (jax.nn.silu(h_gate) * h_up).astype(jnp.bfloat16)
        out_rows = jnp.dot(hidden, wd_e, preferred_element_type=jnp.float32) * gates_e[:, None]
        return acc_sum.at[rows_e].add(out_rows), None

    acc_init = jnp.zeros((TOKENS, D_MODEL), jnp.float32)
    y_total, _ = lax.scan(add_expert, acc_init, (tok_rows, gate_rows, w_gate, w_up, w_down))
    return y_total.astype(jnp.bfloat16)
```

```python
import functools

import jax
import jax.numpy as jnp
from jax import lax
from jax.experimental import pallas as pl
from jax.experimental.pallas import tpu as pltpu
from jax.sharding import PartitionSpec as P

MESH = pl.DeviceIdType.MESH
NK = 4
CW = 256
GRP = 4
SLOTS = 8
ROWS = 64
TOPK = 6


def moe_kernel(x_ref, ids_ref, gate_ref, wg, wu, wd, out_ref,
               xall, xg, meta, pmat, cmat, gbuf, acc_a, acc_b, hbuf, obuf,
               wgs, wus, wds, pown, psib, rd, rfar, rnear, ry,
               ags, agr, mss, msr, wsem, wdsem,
               ds_s, ds_r, fs_s, fs_r, ns_s, ns_r, ys_s, ys_r):
    f32, bf16 = jnp.float32, jnp.bfloat16
    d_model = x_ref.shape[1]
    kw = d_model // NK
    nc = d_model // CW
    n_exp = wg.shape[0]
    n_grp = n_exp // GRP

    z = lax.axis_index("tp")
    ep = lax.axis_index("ep")
    y = ep // 2
    c = ep % 2
    zn = (z + 1) % 4
    zq = (z + 3) % 4
    zo = (z + 2) % 4
    sib = {"ep": 2 * y + 1 - c}
    yn = {"ep": 2 * (1 - y) + c}
    zp = {"tp": zn}
    zm = {"tp": zq}
    sends = []

    def rcopy(src, dst, ssem, rsem, dev):
        return pltpu.make_async_remote_copy(src_ref=src, dst_ref=dst, send_sem=ssem, recv_sem=rsem,
                                            device_id=dev, device_id_type=MESH)

    def send(*args):
        copy = rcopy(*args)
        copy.start()
        sends.append(copy)

    def w_copies(k, g):
        rows = pl.ds(g * GRP, GRP)
        cols = pl.ds(k * kw, kw)
        return (pltpu.make_async_copy(wg.at[rows, cols, :], wgs.at[g], wsem.at[0, g]),
                pltpu.make_async_copy(wu.at[rows, cols, :], wus.at[g], wsem.at[1, g]))

    def wd_copy(n, g):
        rows = pl.ds(g * GRP, GRP)
        return pltpu.make_async_copy(wd.at[rows, :, pl.ds(n * CW, CW)], wds.at[n % 2, rows], wdsem.at[n % 2, g])

    for g in range(n_grp):
        for copy in w_copies(0, g):
            copy.start()
    for n in range(2):
        for g in range(n_grp):
            wd_copy(n, g).start()

    barrier = pltpu.get_barrier_semaphore()
    peers = [{"ep": (ep + d // 4) % 4, "tp": (z + d % 4) % 4} for d in range(1, 16)]
    for peer in peers:
        pl.semaphore_signal(barrier, inc=1, device_id=peer, device_id_type=MESH)
    pl.semaphore_wait(barrier, 15)

    def idx(cc, yy, zz):
        return cc * 8 + yy * 4 + zz

    me = idx(c, y, z)

    def send_block(k, slot, b, dev):
        src = x_ref.at[:, pl.ds(k * kw, kw)] if b is me else xall.at[k, b]
        send(src, xall.at[k, b], ags.at[k, slot], agr.at[k, b], dev)

    def wait_block(k, b):
        rcopy(xall.at[k, b], xall.at[k, b], ags.at[k, 0], agr.at[k, b], sib).wait_recv()

    y_own = idx(c, 1 - y, z)

    def step_f_own(k):
        send_block(k, 2, me, zp)
        send_block(k, 3, me, zm)
        send_block(k, 1, me, sib)

    def step_f_other(k):
        wait_block(k, y_own)
        send_block(k, 4, y_own, zp)
        send_block(k, 5, y_own, zm)
        send_block(k, 6, y_own, sib)

    def step_a(k):
        b = idx(c, y, zq)
        wait_block(k, b)
        send_block(k, 7, b, zp)
        send_block(k, 9, b, sib)
        b = idx(c, 1 - y, zn)
        wait_block(k, b)
        send_block(k, 8, b, zm)
        send_block(k, 10, b, sib)
        b = idx(c, y, zn)
        wait_block(k, b)
        send_block(k, 11, b, sib)
        b = idx(c, 1 - y, zq)
        wait_block(k, b)
        send_block(k, 12, b, sib)

    def step_b(k):
        b = idx(c, y, zo)
        wait_block(k, b)
        send_block(k, 13, b, sib)
        b = idx(c, 1 - y, zo)
        wait_block(k, b)
        send_block(k, 14, b, sib)

    def wait_sibling(k):
        for b in range(8):
            wait_block(k, (1 - c) * 8 + b)

    send_block(0, 0, me, yn)
    step_f_own(0)
    for k in range(1, NK):
        send_block(k, 0, me, yn)

    lane = lax.broadcasted_iota(jnp.int32, (128, 128), 1)
    sub = lax.broadcasted_iota(jnp.int32, (128, 128), 0)
    tri = jnp.where((sub < lane % ROWS) & (sub < ROWS), 1.0, 0.0).astype(bf16)

    def flip(v):
        v = jnp.concatenate([v, jnp.zeros((ROWS, 128 - TOPK), f32)], axis=1)
        v = jnp.concatenate([v, v], axis=0)
        return v.T[:8]

    ids_t = flip(ids_ref[...].astype(f32))
    gate_t = flip(gate_ref[...])
    exp_id = lax.broadcasted_iota(jnp.int32, (64, 128), 0).astype(f32)
    hits = [jnp.where(exp_id == ids_t[j:j + 1], 1.0, 0.0) for j in range(TOPK)]
    chosen = functools.reduce(lambda p, q: p + q, hits)
    rank = jnp.dot(chosen.astype(bf16), tri, preferred_element_type=f32)
    code = [SLOTS * ids_t[j:j + 1] + jnp.sum(rank * hits[j], axis=0, keepdims=True) for j in range(TOPK)]
    code = jnp.concatenate(code + [jnp.full((8 - TOPK, 128), -1.0, f32)], axis=0)
    meta[me, 0:8, :] = code
    meta[me, 8:16, :] = gate_t
    for k in range(NK):
        xall[k, me] = x_ref[:, k * kw:(k + 1) * kw]
    for d, peer in enumerate(peers):
        send(meta.at[me], meta.at[me], mss.at[d], msr.at[me], peer)

    step_f_other(0)
    step_a(0)
    if NK > 1:
        step_f_own(1)
        step_f_other(1)

    for d in range(1, 16):
        s_ep, s_z = (ep + d // 4) % 4, (z + d % 4) % 4
        b = idx(s_ep % 2, s_ep // 2, s_z)
        rcopy(meta.at[b], meta.at[b], mss.at[0], msr.at[b], sib).wait_recv()

    def build(p, carry):
        half = lax.broadcasted_iota(jnp.int32, (8, 128), 1) < ROWS
        both = jnp.where(half, meta[2 * p, 0:8, :], meta[2 * p + 1, 0:8, :]).astype(jnp.int32)
        gts = jnp.where(half, meta[2 * p, 8:16, :], meta[2 * p + 1, 8:16, :])
        expert = lax.shift_right_arithmetic(both, 3)
        slot = both - expert * SLOTS
        row = (expert - ep * n_exp) * (2 * SLOTS) + jnp.where(half, 0, SLOTS) + slot
        r = lax.broadcasted_iota(jnp.int32, (n_exp * 2 * SLOTS, 128), 0)
        sel = jnp.zeros(r.shape, f32)
        wts = jnp.zeros(r.shape, f32)
        for j in range(TOPK):
            eq = r == row[j:j + 1]
            sel = jnp.where(eq, 1.0, sel)
            wts = jnp.where(eq, gts[j:j + 1], wts)
        pmat[p] = sel.astype(bf16)
        selt = sel.T.astype(bf16)
        cmat[p] = jnp.concatenate([selt, selt, selt], axis=1)
        per_row = jnp.broadcast_to(jnp.sum(wts, axis=1, keepdims=True), wts.shape)
        for e in range(n_exp):
            gbuf[e, pl.ds(p * 16, 16), :] = per_row[e * 16:(e + 1) * 16]
        return carry

    lax.fori_loop(0, 8, build, 0)
    step_b(0)

    def compute(k):
        def gather(i, carry):
            for u in range(2):
                p = i * 2 + u
                rows = xall[k, pl.ds(2 * p, 2)].reshape(2 * ROWS, kw)
                v = jnp.dot(pmat[p], rows, preferred_element_type=f32).astype(bf16)
                for e in range(n_exp):
                    xg[e, pl.ds(p * 16, 16), :] = v[e * 16:(e + 1) * 16]
            return carry

        lax.fori_loop(0, 4, gather, 0)

        def experts(g, carry):
            for copy in w_copies(k, g):
                copy.wait()
            for u in range(GRP):
                e = g * GRP + u
                xe = xg[e]
                a = jnp.dot(xe, wgs[g, u], preferred_element_type=f32)
                b = jnp.dot(xe, wus[g, u], preferred_element_type=f32)
                if k > 0:
                    a = acc_a[e] + a
                    b = acc_b[e] + b
                if k < NK - 1:
                    acc_a[e] = a
                    acc_b[e] = b
                else:
                    hbuf[e] = (jax.nn.silu(a) * b).astype(bf16)
            if k < NK - 1:
                for copy in w_copies(k + 1, g):
                    copy.start()
            return carry

        lax.fori_loop(0, n_grp, experts, 0)

    for k in range(NK):
        if k + 1 < NK:
            step_a(k + 1)
        if k + 2 < NK:
            step_f_own(k + 2)
            step_f_other(k + 2)
        wait_sibling(k)
        compute(k)
        if k + 1 < NK:
            step_b(k + 1)

    def down(n):
        def body(g, carry):
            wd_copy(n, g).wait()
            for u in range(GRP):
                e = g * GRP + u
                o = jnp.dot(hbuf[e], wds[n % 2, e], preferred_element_type=f32)
                gt = gbuf[e]
                o = o * jnp.concatenate([gt] * (CW // 128), axis=1)
                parts = []
                for i in range(3):
                    part = o.astype(bf16)
                    if i < 2:
                        o = o - part.astype(f32)
                    parts.append(part)
                for p in range(8):
                    for i in range(3):
                        obuf[pl.ds(p * 768 + i * 256 + e * 16, 16), :] = parts[i][p * 16:(p + 1) * 16]
            return carry

        lax.fori_loop(0, n_grp, body, 0)
        if n + 2 < nc:
            for g in range(n_grp):
                wd_copy(n + 2, g).start()

    def merged(p):
        v = jnp.dot(cmat[p], obuf[pl.ds(p * 768, 768), :], preferred_element_type=f32)
        return v.reshape(2, ROWS, CW)

    sib_sends = {}

    def combine(n):
        if n >= 2:
            for copy in sib_sends.pop(n - 2):
                copy.wait_send()
        out = []
        for q in range(4):
            psib[n % 2, 2 * q:2 * q + 2] = merged((1 - c) * 4 + q)
        for q in range(4):
            copy = rcopy(psib.at[n % 2, pl.ds(2 * q, 2)], rd.at[n, pl.ds(2 * q, 2)], ds_s.at[n, q], ds_r.at[n, q], sib)
            copy.start()
            out.append(copy)
        sib_sends[n] = out
        for q in range(4):
            pown[n, 2 * q:2 * q + 2] = merged(c * 4 + q)

    def piece(n, h, zd):
        if n % 2 == 0:
            return pown.at[n, h * 4 + zd]
        return pown.at[n, y * 4 + zd, pl.ds(h * 32, 32)]

    def half_buf(buf, n, i):
        if n % 2 == 0:
            return buf.at[n, i]
        return buf.at[n, i, pl.ds(0, 32)]

    def z_first_sends(n):
        send(piece(n, 0, zo), half_buf(rfar, n, 0), fs_s.at[n, 0], fs_r.at[n, 0], zm)
        send(piece(n, 1, zo), half_buf(rfar, n, 1), fs_s.at[n, 1], fs_r.at[n, 1], zp)
        send(piece(n, 1, zq), half_buf(rnear, n, 0), ns_s.at[n, 0], ns_r.at[n, 0], zm)
        send(piece(n, 0, zn), half_buf(rnear, n, 1), ns_s.at[n, 1], ns_r.at[n, 1], zp)

    def z_second_sends(n):
        for i, zd, dev in ((0, zq, zm), (1, zn, zp)):
            buf = half_buf(rfar, n, i)
            rcopy(buf, buf, fs_s.at[n, i], fs_r.at[n, i], sib).wait_recv()
            dst = piece(n, i, zd)
            dst[...] = dst[...] + buf[...]
        for i, zd, dev in ((0, zq, zm), (1, zn, zp)):
            send(piece(n, i, zd), half_buf(rnear, n, 2 + i), ns_s.at[n, 2 + i], ns_r.at[n, 2 + i], dev)

    def z_total(n):
        for i in range(4):
            buf = half_buf(rnear, n, i)
            rcopy(buf, buf, ns_s.at[n, i], ns_r.at[n, i], sib).wait_recv()
        for h, i, j in ((0, 1, 2), (1, 0, 3)):
            dst = piece(n, h, z)
            dst[...] = dst[...] + half_buf(rnear, n, i)[...] + half_buf(rnear, n, j)[...]

    def core_total(n):
        for q in range(4):
            buf = rd.at[n, pl.ds(2 * q, 2)]
            rcopy(buf, buf, ds_s.at[n, q], ds_r.at[n, q], sib).wait_recv()
            pown[n, 2 * q:2 * q + 2] = pown[n, 2 * q:2 * q + 2] + rd[n, 2 * q:2 * q + 2]

    def y_buf(n):
        return ry.at[n, pl.ds(0, 1)] if n % 2 == 0 else ry.at[n]

    def y_src(n):
        return pown.at[n, pl.ds((1 - y) * 4 + z, 1)] if n % 2 == 0 else pown.at[n, pl.ds((1 - y) * 4, 4)]

    def y_send(n):
        send(y_src(n), y_buf(n), ys_s.at[n], ys_r.at[n], yn)

    def y_wait(n):
        rcopy(y_buf(n), y_buf(n), ys_s.at[n], ys_r.at[n], sib).wait_recv()

    def finish(n, v):
        out_ref[:, n * CW:(n + 1) * CW] = v.astype(bf16)

    def stage(n, j):
        if n % 2 == 0:
            if j == 0:
                core_total(n)
                z_first_sends(n)
            elif j == 1:
                z_second_sends(n)
            elif j == 2:
                z_total(n)
                y_send(n)
            else:
                y_wait(n)
                finish(n, pown[n, y * 4 + z] + ry[n, 0])
        else:
            if j == 0:
                core_total(n)
                y_send(n)
            elif j == 1:
                y_wait(n)
                own = pown.at[n, pl.ds(y * 4, 4)]
                own[...] = own[...] + ry[n]
                z_first_sends(n)
            elif j == 2:
                z_second_sends(n)
            else:
                z_total(n)
                finish(n, pown[n, y * 4 + z])

    for t in range(nc + 3):
        if t < nc:
            down(t)
            combine(t)
        for j in range(4):
            if 0 <= t - j < nc:
                stage(t - j, j)

    for out in sib_sends.values():
        for copy in out:
            copy.wait_send()
    for copy in sends:
        copy.wait_send()


def solution(mesh):
    row_spec = P(("dp", "ep", "tp"), None)

    def local_moe(x, ids, gates, wg, wu, wd):
        rows, d_model = x.shape
        n_exp, _, ff = wg.shape
        nc = d_model // CW
        kw = d_model // NK
        f32, bf16 = jnp.float32, jnp.bfloat16
        vm, dma = pltpu.VMEM, pltpu.SemaphoreType.DMA
        whole = pl.BlockSpec(memory_space=pltpu.VMEM)
        far = pl.BlockSpec(memory_space=pl.ANY)
        return pl.pallas_call(
            moe_kernel,
            out_shape=jax.ShapeDtypeStruct((rows, d_model), bf16),
            in_specs=[whole, whole, whole, far, far, far],
            out_specs=whole,
            scratch_shapes=[
                vm((NK, 16, rows, kw), bf16),
                vm((n_exp, 128, kw), bf16),
                vm((16, 16, 128), f32),
                vm((8, 256, 128), bf16),
                vm((8, 128, 768), bf16),
                vm((n_exp, 128, 128), f32),
                vm((n_exp, 128, ff), f32),
                vm((n_exp, 128, ff), f32),
                vm((n_exp, 128, ff), bf16),
                vm((8 * 768, CW), bf16),
                vm((n_exp // GRP, GRP, kw, ff), bf16),
                vm((n_exp // GRP, GRP, kw, ff), bf16),
                vm((2, n_exp, ff, CW), bf16),
                vm((nc, 8, rows, CW), f32),
                vm((2, 8, rows, CW), f32),
                vm((nc, 8, rows, CW), f32),
                vm((nc, 2, rows, CW), f32),
                vm((nc, 4, rows, CW), f32),
                vm((nc, 4, rows, CW), f32),
                dma((NK, 15)), dma((NK, 16)), dma((15,)), dma((16,)),
                dma((2, n_exp // GRP)), dma((2, n_exp // GRP)),
                dma((nc, 4)), dma((nc, 4)), dma((nc, 2)), dma((nc, 2)),
                dma((nc, 4)), dma((nc, 4)), dma((nc,)), dma((nc,)),
            ],
            compiler_params=pltpu.CompilerParams(
                collective_id=0, has_side_effects=True, vmem_limit_bytes=66_000_000),
        )(x, ids, gates, wg, wu, wd)

    return jax.shard_map(
        local_moe, mesh=mesh,
        in_specs=(row_spec, row_spec, row_spec, P("ep", None, "tp"), P("ep", None, "tp"), P("ep", "tp", None)),
        out_specs=row_spec, check_vma=False)
```

```python
import functools

import jax
import jax.numpy as jnp
from jax import lax
from jax.experimental import pallas as pl
from jax.experimental.pallas import tpu as pltpu
from jax.sharding import PartitionSpec as P

MESH = pl.DeviceIdType.MESH
NK = 4
CW = 256
GRP = 4
SLOTS = 8
ROWS = 64
TOPK = 6
FLIP = True
ZFIRST = (1,)


def moe_kernel(x_ref, ids_ref, gate_ref, wg, wu, wd, out_ref,
               xall, xg, meta, pmat, cmat, gbuf, acc_a, acc_b, hbuf, obuf,
               wgs, wus, wds, pown, psib, rd, rr, rl, rr2, rl2, ry,
               ags, agr, mss, msr, wsem, wdsem,
               ds_s, ds_r, rr_s, rr_r, rl_s, rl_r, ys_s, ys_r):
    f32, bf16 = jnp.float32, jnp.bfloat16
    d_model = x_ref.shape[1]
    kw = d_model // NK
    nc = d_model // CW
    n_exp = wg.shape[0]
    n_grp = n_exp // GRP

    z = lax.axis_index("tp")
    ep = lax.axis_index("ep")
    y = ep // 2
    c = ep % 2
    sib = {"ep": 2 * y + 1 - c}
    yn = {"ep": 2 * (1 - y) + c}
    sends = []
    hops = []

    def rcopy(src, dst, ssem, rsem, dev):
        return pltpu.make_async_remote_copy(src_ref=src, dst_ref=dst, send_sem=ssem, recv_sem=rsem,
                                            device_id=dev, device_id_type=MESH)

    def send(*args):
        copy = rcopy(*args)
        copy.start()
        sends.append(copy)

    def w_copies(k, g):
        rows = pl.ds(g * GRP, GRP)
        cols = pl.ds(k * kw, kw)
        return (pltpu.make_async_copy(wg.at[rows, :, cols], wgs.at[g], wsem.at[0, g]),
                pltpu.make_async_copy(wu.at[rows, :, cols], wus.at[g], wsem.at[1, g]))

    def wd_copy(n, g):
        rows = pl.ds(g * GRP, GRP)
        return pltpu.make_async_copy(wd.at[rows, :, pl.ds(n * CW, CW)], wds.at[n % 2, rows], wdsem.at[n % 2, g])

    for g in range(n_grp):
        for copy in w_copies(0, g):
            copy.start()
    for n in range(2):
        for g in range(n_grp):
            wd_copy(n, g).start()

    barrier = pltpu.get_barrier_semaphore()
    peers = [{"ep": (ep + d // 4) % 4, "tp": (z + d % 4) % 4} for d in range(1, 16)]
    for peer in peers:
        pl.semaphore_signal(barrier, inc=1, device_id=peer, device_id_type=MESH)
    pl.semaphore_wait(barrier, 15)

    def idx(cc, yy, zz):
        return cc * 8 + yy * 4 + zz

    me = idx(c, y, z)

    def send_block(k, slot, b, dev):
        src = x_ref.at[:, pl.ds(k * kw, kw)] if b is me else xall.at[k, b]
        send(src, xall.at[k, b], ags.at[k, slot], agr.at[k, b], dev)

    def wait_block(k, b):
        rcopy(xall.at[k, b], xall.at[k, b], ags.at[k, 0], agr.at[k, b], sib).wait_recv()

    def z_block(k, i):
        return rcopy(x_ref.at[:, pl.ds(k * kw, kw)], xall.at[k, me], ags.at[k, i], agr.at[k, me],
                     {"tp": (z + i) % 4})

    def relay(k):
        b = idx(c, y, 3 * (2 - z))
        return rcopy(xall.at[k, b], xall.at[k, b], ags.at[k, 15], agr.at[k, b], {"tp": 3 * (z - 1)})

    inner = (z == 1) | (z == 2)
    near = {1: z < 3, 2: None, 3: z > 0}

    def send_z(k):
        for i in (2, 1, 3):
            if near[i] is None:
                copy = z_block(k, i)
                copy.start()
                sends.append(copy)
            else:
                pl.when(near[i])(lambda: z_block(k, i).start())
                hops.append((near[i], [functools.partial(z_block, k, i)]))

    def send_own(k):
        send_block(k, 0, me, yn)
        send_block(k, 4, me, sib)

    def step_a(k):
        for i in (2, 1, 3):
            b = idx(c, y, (z + i) % 4)
            wait_block(k, b)
            if i == 2:
                pl.when(inner)(lambda: relay(k).start())
                hops.append((inner, [functools.partial(relay, k)]))
                if k + 1 < NK:
                    send_z(k + 1)
            send_block(k, 4 + i, b, yn)
            send_block(k, 7 + i, b, sib)
        if k + 2 < NK:
            send_own(k + 2)

    def step_b(k):
        for i in range(4):
            b = idx(c, 1 - y, (z + i) % 4)
            wait_block(k, b)
            send_block(k, 11 + i, b, sib)

    def wait_sibling(k):
        for b in range(8):
            wait_block(k, (1 - c) * 8 + b)

    send_z(0)
    send_own(0)

    lane = lax.broadcasted_iota(jnp.int32, (128, 128), 1)
    sub = lax.broadcasted_iota(jnp.int32, (128, 128), 0)
    tri = jnp.where((sub < lane % ROWS) & (sub < ROWS), 1.0, 0.0).astype(bf16)

    def twice(v):
        v = jnp.concatenate([v, v], axis=1)
        return jnp.concatenate([v, jnp.zeros((8 - TOPK, 128), f32)], axis=0)

    ids_t = twice(ids_ref[...].astype(f32))
    gate_t = twice(gate_ref[...])
    exp_id = lax.broadcasted_iota(jnp.int32, (64, 128), 0).astype(f32)
    hits = [jnp.where(exp_id == ids_t[j:j + 1], 1.0, 0.0) for j in range(TOPK)]
    chosen = functools.reduce(lambda p, q: p + q, hits)
    rank = jnp.dot(chosen.astype(bf16), tri, preferred_element_type=f32)
    code = [SLOTS * ids_t[j:j + 1] + jnp.sum(rank * hits[j], axis=0, keepdims=True) for j in range(TOPK)]
    code = jnp.concatenate(code + [jnp.full((8 - TOPK, 128), -1.0, f32)], axis=0)
    meta[me, 0:8, :] = code
    meta[me, 8:16, :] = gate_t
    for k in range(NK):
        xall[k, me] = x_ref[:, k * kw:(k + 1) * kw]
    for d, peer in enumerate(peers):
        send(meta.at[me], meta.at[me], mss.at[d], msr.at[me], peer)
    if NK > 1:
        send_own(1)

    step_a(0)

    for d in range(1, 16):
        s_ep, s_z = (ep + d // 4) % 4, (z + d % 4) % 4
        b = idx(s_ep % 2, s_ep // 2, s_z)
        rcopy(meta.at[b], meta.at[b], mss.at[0], msr.at[b], sib).wait_recv()

    def build(p, carry):
        half = lax.broadcasted_iota(jnp.int32, (8, 128), 1) < ROWS
        both = jnp.where(half, meta[2 * p, 0:8, :], meta[2 * p + 1, 0:8, :]).astype(jnp.int32)
        gts = jnp.where(half, meta[2 * p, 8:16, :], meta[2 * p + 1, 8:16, :])
        expert = lax.shift_right_arithmetic(both, 3)
        slot = both - expert * SLOTS
        row = (expert - ep * n_exp) * (2 * SLOTS) + jnp.where(half, 0, SLOTS) + slot
        r = lax.broadcasted_iota(jnp.int32, (n_exp * 2 * SLOTS, 128), 0)
        sel = jnp.zeros(r.shape, f32)
        wts = jnp.zeros(r.shape, f32)
        for j in range(TOPK):
            eq = r == row[j:j + 1]
            sel = jnp.where(eq, 1.0, sel)
            wts = jnp.where(eq, gts[j:j + 1], wts)
        pmat[p] = sel.astype(bf16)
        selt = sel.T.astype(bf16)
        cmat[p] = jnp.concatenate([selt, selt, selt], axis=1)
        per_row = jnp.broadcast_to(jnp.sum(wts, axis=1, keepdims=True), wts.shape)
        for e in range(n_exp):
            gbuf[e, pl.ds(p * 16, 16), :] = per_row[e * 16:(e + 1) * 16]
        return carry

    lax.fori_loop(0, 8, build, 0)
    if NK > 1:
        step_a(1)
    step_b(0)

    def proj(w, xe):
        dims = (((1,), (1,)), ((), ()))
        if FLIP:
            return lax.dot_general(w, xe, dims, preferred_element_type=f32)
        return lax.dot_general(xe, w, dims, preferred_element_type=f32)

    def compute(k, between):
        def gather(i, carry):
            for u in range(2):
                p = i * 2 + u
                rows = xall[k, pl.ds(2 * p, 2)].reshape(2 * ROWS, kw)
                v = jnp.dot(pmat[p], rows, preferred_element_type=f32).astype(bf16)
                for e in range(n_exp):
                    xg[e, pl.ds(p * 16, 16), :] = v[e * 16:(e + 1) * 16]
            return carry

        lax.fori_loop(0, 4, gather, 0)

        def experts(g, carry):
            for copy in w_copies(k, g):
                copy.wait()
            for u in range(GRP):
                e = g * GRP + u
                xe = xg[e]
                a = proj(wgs[g, u], xe)
                b = proj(wus[g, u], xe)
                if k > 0:
                    a = acc_a[e] + a
                    b = acc_b[e] + b
                if k < NK - 1:
                    acc_a[e] = a
                    acc_b[e] = b
                else:
                    h = jax.nn.silu(a) * b
                    hbuf[e] = (h.T if FLIP else h).astype(bf16)
            if k < NK - 1:
                for copy in w_copies(k + 1, g):
                    copy.start()
            return carry

        lax.fori_loop(0, n_grp // 2, experts, 0)
        between()
        lax.fori_loop(n_grp // 2, n_grp, experts, 0)

    for k in range(NK):
        wait_sibling(k)
        compute(k, functools.partial(step_a, k + 2) if k + 2 < NK else lambda: None)
        if k + 1 < NK:
            step_b(k + 1)

    def down(n):
        def body(g, carry):
            wd_copy(n, g).wait()
            for u in range(GRP):
                e = g * GRP + u
                o = jnp.dot(hbuf[e], wds[n % 2, e], preferred_element_type=f32)
                gt = gbuf[e]
                o = o * jnp.concatenate([gt] * (CW // 128), axis=1)
                parts = []
                for i in range(3):
                    part = o.astype(bf16)
                    if i < 2:
                        o = o - part.astype(f32)
                    parts.append(part)
                for p in range(8):
                    for i in range(3):
                        obuf[pl.ds(p * 768 + i * 256 + e * 16, 16), :] = parts[i][p * 16:(p + 1) * 16]
            return carry

        lax.fori_loop(0, n_grp, body, 0)
        if n + 2 < nc:
            for g in range(n_grp):
                wd_copy(n + 2, g).start()

    def merged(p):
        v = jnp.dot(cmat[p], obuf[pl.ds(p * 768, 768), :], preferred_element_type=f32)
        return v.reshape(2, ROWS, CW)

    def part(ref, n, q):
        return ref.at[n, pl.ds(2 * (q % 2), 2), q // 2]

    sib_sends = {}

    def combine(n):
        if n >= 2:
            for copy in sib_sends.pop(n - 2):
                copy.wait_send()
        out = []
        for q in range(4):
            part(psib, n % 2, q)[...] = merged((1 - c) * 4 + q)
        for q in range(4):
            copy = rcopy(part(psib, n % 2, q), part(rd, n, q), ds_s.at[n, q], ds_r.at[n, q], sib)
            copy.start()
            out.append(copy)
        sib_sends[n] = out
        for q in range(4):
            part(pown, n, q)[...] = merged(c * 4 + q)

    def add(dst, src):
        dst[...] = dst[...] + src[...]

    def core_total(n):
        for q in range(4):
            buf = part(rd, n, q)
            rcopy(buf, buf, ds_s.at[n, q], ds_r.at[n, q], sib).wait_recv()
            add(part(pown, n, q), buf)

    def piece(n, d):
        return pown.at[n, d] if n in ZFIRST else pown.at[n, d, y]

    def r_buf(n, d):
        return rr2.at[ZFIRST.index(n), d] if n in ZFIRST else rr.at[n, d]

    def l_buf(n, d):
        return rl2.at[ZFIRST.index(n), d] if n in ZFIRST else rl.at[n, d]

    def hop(n, at, right):
        buf, ssem, rsem = (r_buf, rr_s, rr_r) if right else (l_buf, rl_s, rl_r)
        dests = range(3, at, -1) if right else range(0, at)
        here = z == at

        def onward(n, d):
            return rcopy(piece(n, d), buf(n, d), ssem.at[n, d], rsem.at[n, d],
                         {"tp": (z + (1 if right else 3)) % 4})

        @pl.when(here)
        def _():
            for d in dests:
                if 0 < at < 3:
                    rcopy(buf(n, d), buf(n, d), ssem.at[n, d], rsem.at[n, d], sib).wait_recv()
                    add(piece(n, d), buf(n, d))
                onward(n, d).start()

        hops.append((here, [functools.partial(onward, n, d) for d in dests]))

    def z_total(n):
        @pl.when(z > 0)
        def _():
            rcopy(r_buf(n, z), r_buf(n, z), rr_s.at[n, z], rr_r.at[n, z], sib).wait_recv()
            add(piece(n, z), r_buf(n, z))

        @pl.when(z < 3)
        def _():
            rcopy(l_buf(n, z), l_buf(n, z), rl_s.at[n, z], rl_r.at[n, z], sib).wait_recv()
            add(piece(n, z), l_buf(n, z))

    def y_buf(n):
        return ry.at[n, pl.ds(0, 1)] if n in ZFIRST else ry.at[n]

    def y_send(n):
        src = pown.at[n, pl.ds(z, 1), 1 - y] if n in ZFIRST else pown.at[n, :, 1 - y]
        send(src, y_buf(n), ys_s.at[n], ys_r.at[n], yn)

    def y_add(n):
        rcopy(y_buf(n), y_buf(n), ys_s.at[n], ys_r.at[n], sib).wait_recv()
        add(pown.at[n, pl.ds(z, 1), y] if n in ZFIRST else pown.at[n, :, y], y_buf(n))

    def finish(n):
        out_ref[:, n * CW:(n + 1) * CW] = pown[n, z, y].astype(bf16)

    def y_hop(n):
        y_add(n)
        hop(n, 0, True)
        hop(n, 3, False)

    def hop_1(n):
        hop(n, 1, True)
        hop(n, 2, False)

    def hop_2(n):
        hop(n, 2, True)
        hop(n, 1, False)

    def z_end(n):
        z_total(n)
        if n in ZFIRST:
            y_send(n)
        else:
            finish(n)

    def y_end(n):
        y_add(n)
        finish(n)

    def first(n):
        core_total(n)
        if n in ZFIRST:
            hop(n, 0, True)
            hop(n, 3, False)
        else:
            y_send(n)

    stages = {False: {2: y_hop, 3: hop_1, 4: hop_2, 5: z_end},
              True: {2: hop_1, 3: hop_2, 4: z_end, 6: y_end}}
    for t in range(nc + 6):
        if t < nc:
            down(t)
            combine(t)
        for lag in range(6, 0, -1):
            n = t - lag
            if 0 <= n < nc and lag in stages[n in ZFIRST]:
                stages[n in ZFIRST][lag](n)
        if t < nc:
            first(t)

    for out in sib_sends.values():
        for copy in out:
            copy.wait_send()
    for copy in sends:
        copy.wait_send()
    for here, makers in hops:
        @pl.when(here)
        def _():
            for maker in makers:
                maker().wait_send()


def solution(mesh):
    row_spec = P(("dp", "ep", "tp"), None)

    def local_moe(x, ids, gates, wg, wu, wd):
        rows, d_model = x.shape
        n_exp, _, ff = wg.shape
        nc = d_model // CW
        kw = d_model // NK
        f32, bf16 = jnp.float32, jnp.bfloat16
        vm, dma = pltpu.VMEM, pltpu.SemaphoreType.DMA
        whole = pl.BlockSpec(memory_space=pltpu.VMEM)
        far = pl.BlockSpec(memory_space=pl.ANY)
        return pl.pallas_call(
            moe_kernel,
            out_shape=jax.ShapeDtypeStruct((rows, d_model), bf16),
            in_specs=[whole, whole, whole, far, far, far],
            out_specs=whole,
            scratch_shapes=[
                vm((NK, 16, rows, kw), bf16),
                vm((n_exp, 128, kw), bf16),
                vm((16, 16, 128), f32),
                vm((8, 256, 128), bf16),
                vm((8, 128, 768), bf16),
                vm((n_exp, 128, 128), f32),
                vm((n_exp, ff, 128) if FLIP else (n_exp, 128, ff), f32),
                vm((n_exp, ff, 128) if FLIP else (n_exp, 128, ff), f32),
                vm((n_exp, 128, ff), bf16),
                vm((8 * 768, CW), bf16),
                vm((n_exp // GRP, GRP, ff, kw), bf16),
                vm((n_exp // GRP, GRP, ff, kw), bf16),
                vm((2, n_exp, ff, CW), bf16),
                vm((nc, 4, 2, rows, CW), f32),
                vm((2, 4, 2, rows, CW), f32),
                vm((nc, 4, 2, rows, CW), f32),
                vm((nc, 4, rows, CW), f32),
                vm((nc, 4, rows, CW), f32),
                vm((len(ZFIRST), 4, 2, rows, CW), f32),
                vm((len(ZFIRST), 4, 2, rows, CW), f32),
                vm((nc, 4, rows, CW), f32),
                dma((NK, 16)), dma((NK, 16)), dma((15,)), dma((16,)),
                dma((2, n_exp // GRP)), dma((2, n_exp // GRP)),
                dma((nc, 4)), dma((nc, 4)), dma((nc, 4)), dma((nc, 4)),
                dma((nc, 4)), dma((nc, 4)), dma((nc,)), dma((nc,)),
            ],
            compiler_params=pltpu.CompilerParams(
                collective_id=0, has_side_effects=True, vmem_limit_bytes=66_000_000),
        )(x, ids.T, gates.T, wg.swapaxes(1, 2), wu.swapaxes(1, 2), wd)

    return jax.shard_map(
        local_moe, mesh=mesh,
        in_specs=(row_spec, row_spec, row_spec, P("ep", None, "tp"), P("ep", None, "tp"), P("ep", "tp", None)),
        out_specs=row_spec, check_vma=False)
```

```python
import functools

import jax
import jax.numpy as jnp
from jax import lax
from jax.experimental import pallas as pl
from jax.experimental.pallas import tpu as pltpu
from jax.sharding import PartitionSpec as P

MESH = pl.DeviceIdType.MESH
NK = 8
STEPS = ((0, 1), (1, 2), (3, 2), (5, 2), (7, 1))
CW = 256
WIDTHS = (256,) * 8
GRP = 8
SLOTS = 8
ROWS = 64
TOPK = 6
AHEAD = 3
FLIP = True
DIRECT = (7,)
ZFIRST = (1,)


def moe_kernel(x_ref, ids_ref, gate_ref, wg, wu, wd, out_ref,
               xall, xg, meta, pmat, cmat, gbuf, acc_a, acc_b, hbuf, obuf,
               wgs, wus, wds, pown, psib, rd, rr, rl, rr2, rl2, ry,
               ags, agr, mss, msr, wsem, wdsem,
               ds_s, ds_r, rr_s, rr_r, rl_s, rl_r, ys_s, ys_r):
    f32, bf16 = jnp.float32, jnp.bfloat16
    d_model = x_ref.shape[1]
    kw = d_model // NK
    nc = len(WIDTHS)
    starts = [sum(WIDTHS[:n]) for n in range(nc)]
    n_exp = wg.shape[0]
    n_grp = n_exp // GRP

    z = lax.axis_index("tp")
    ep = lax.axis_index("ep")
    y = ep // 2
    c = ep % 2
    sib = {"ep": 2 * y + 1 - c}
    yn = {"ep": 2 * (1 - y) + c}
    sends = []
    hops = []

    def rcopy(src, dst, ssem, rsem, dev):
        return pltpu.make_async_remote_copy(src_ref=src, dst_ref=dst, send_sem=ssem, recv_sem=rsem,
                                            device_id=dev, device_id_type=MESH)

    def send(*args):
        copy = rcopy(*args)
        copy.start()
        sends.append(copy)

    def w_copies(s, g):
        rows = pl.ds(g * GRP, GRP)
        cols = pl.ds(STEPS[s][0] * kw, STEPS[s][1] * kw)
        here = pl.ds(0, STEPS[s][1] * kw)
        return (pltpu.make_async_copy(wg.at[rows, :, cols], wgs.at[g, :, :, here], wsem.at[0, g]),
                pltpu.make_async_copy(wu.at[rows, :, cols], wus.at[g, :, :, here], wsem.at[1, g]))

    def wd_copy(n, g):
        rows = pl.ds(g * GRP, GRP)
        return pltpu.make_async_copy(wd.at[rows, :, pl.ds(starts[n], WIDTHS[n])],
                                     wds.at[n % 2, rows, :, pl.ds(0, WIDTHS[n])], wdsem.at[n % 2, g])

    for g in range(n_grp):
        for copy in w_copies(0, g):
            copy.start()
    for n in range(2):
        for g in range(n_grp):
            wd_copy(n, g).start()

    barrier = pltpu.get_barrier_semaphore()
    peers = [{"ep": (ep + d // 4) % 4, "tp": (z + d % 4) % 4} for d in range(1, 16)]
    for peer in peers:
        pl.semaphore_signal(barrier, inc=1, device_id=peer, device_id_type=MESH)
    pl.semaphore_wait(barrier, 15)

    def idx(cc, yy, zz):
        return cc * 8 + yy * 4 + zz

    me = idx(c, y, z)

    def send_block(k, slot, b, dev):
        src = x_ref.at[:, pl.ds(k * kw, kw)] if b is me else xall.at[k, b]
        send(src, xall.at[k, b], ags.at[k, slot], agr.at[k, b], dev)

    def wait_block(k, b):
        rcopy(xall.at[k, b], xall.at[k, b], ags.at[k, 0], agr.at[k, b], sib).wait_recv()

    def z_block(k, i):
        return rcopy(x_ref.at[:, pl.ds(k * kw, kw)], xall.at[k, me], ags.at[k, i], agr.at[k, me],
                     {"tp": (z + i) % 4})

    def relay(k):
        b = idx(c, y, 3 * (2 - z))
        return rcopy(xall.at[k, b], xall.at[k, b], ags.at[k, 15], agr.at[k, b], {"tp": 3 * (z - 1)})

    inner = (z == 1) | (z == 2)
    near = {1: z < 3, 2: None, 3: z > 0}

    def send_z(k):
        for i in (2, 1, 3):
            if near[i] is None:
                copy = z_block(k, i)
                copy.start()
                sends.append(copy)
            else:
                pl.when(near[i])(lambda: z_block(k, i).start())
                hops.append((near[i], [functools.partial(z_block, k, i)]))

    def send_own(k):
        send_block(k, 0, me, yn)
        send_block(k, 4, me, sib)

    def step_a(k):
        for i in (2, 1, 3):
            b = idx(c, y, (z + i) % 4)
            wait_block(k, b)
            if i == 2:
                pl.when(inner)(lambda: relay(k).start())
                hops.append((inner, [functools.partial(relay, k)]))
                if k + AHEAD < NK:
                    send_z(k + AHEAD)
            send_block(k, 4 + i, b, yn)
            send_block(k, 7 + i, b, sib)

    def step_b(k):
        for i in range(4):
            b = idx(c, 1 - y, (z + i) % 4)
            wait_block(k, b)
            send_block(k, 11 + i, b, sib)

    def wait_sibling(k):
        for b in range(8):
            wait_block(k, (1 - c) * 8 + b)

    send_z(0)
    send_own(0)

    lane = lax.broadcasted_iota(jnp.int32, (128, 128), 1)
    sub = lax.broadcasted_iota(jnp.int32, (128, 128), 0)
    tri = jnp.where((sub < lane % ROWS) & (sub < ROWS), 1.0, 0.0).astype(bf16)

    def twice(v):
        v = jnp.concatenate([v, v], axis=1)
        return jnp.concatenate([v, jnp.zeros((8 - TOPK, 128), f32)], axis=0)

    ids_t = twice(ids_ref[...].astype(f32))
    gate_t = twice(gate_ref[...])
    exp_id = lax.broadcasted_iota(jnp.int32, (64, 128), 0).astype(f32)
    hits = [jnp.where(exp_id == ids_t[j:j + 1], 1.0, 0.0) for j in range(TOPK)]
    chosen = functools.reduce(lambda p, q: p + q, hits)
    rank = jnp.dot(chosen.astype(bf16), tri, preferred_element_type=f32)
    code = [SLOTS * ids_t[j:j + 1] + jnp.sum(rank * hits[j], axis=0, keepdims=True) for j in range(TOPK)]
    code = jnp.concatenate(code + [jnp.full((8 - TOPK, 128), -1.0, f32)], axis=0)
    meta[me, 0:8, :] = code
    meta[me, 8:16, :] = gate_t
    for k in range(NK):
        xall[k, me] = x_ref[:, k * kw:(k + 1) * kw]
    for d, peer in enumerate(peers):
        send(meta.at[me], meta.at[me], mss.at[d], msr.at[me], peer)
    for k in range(1, NK):
        if k < AHEAD:
            send_z(k)
        send_own(k)

    step_a(0)

    for d in range(1, 16):
        s_ep, s_z = (ep + d // 4) % 4, (z + d % 4) % 4
        b = idx(s_ep % 2, s_ep // 2, s_z)
        rcopy(meta.at[b], meta.at[b], mss.at[0], msr.at[b], sib).wait_recv()

    def build(p, carry):
        half = lax.broadcasted_iota(jnp.int32, (8, 128), 1) < ROWS
        both = jnp.where(half, meta[2 * p, 0:8, :], meta[2 * p + 1, 0:8, :]).astype(jnp.int32)
        gts = jnp.where(half, meta[2 * p, 8:16, :], meta[2 * p + 1, 8:16, :])
        expert = lax.shift_right_arithmetic(both, 3)
        slot = both - expert * SLOTS
        row = (expert - ep * n_exp) * (2 * SLOTS) + jnp.where(half, 0, SLOTS) + slot
        r = lax.broadcasted_iota(jnp.int32, (n_exp * 2 * SLOTS, 128), 0)
        sel = jnp.zeros(r.shape, f32)
        wts = jnp.zeros(r.shape, f32)
        for j in range(TOPK):
            eq = r == row[j:j + 1]
            sel = jnp.where(eq, 1.0, sel)
            wts = jnp.where(eq, gts[j:j + 1], wts)
        pmat[p] = sel.astype(bf16)
        selt = sel.T.astype(bf16)
        cmat[p] = jnp.concatenate([selt, selt, selt], axis=1)
        per_row = jnp.broadcast_to(jnp.sum(wts, axis=1, keepdims=True), wts.shape)
        gbuf[:, pl.ds(p * 16, 16), :] = per_row.reshape(n_exp, 16, 128)
        return carry

    lax.fori_loop(0, 8, build, 0)

    def proj(w, xe):
        dims = (((1,), (1,)), ((), ()))
        if FLIP:
            return lax.dot_general(w, xe, dims, preferred_element_type=f32)
        return lax.dot_general(xe, w, dims, preferred_element_type=f32)

    def compute(s, *between):
        k0, count = STEPS[s]
        width = count * kw

        def gather(i, carry):
            for u in range(2):
                p = i * 2 + u
                for j in range(count):
                    rows = xall[k0 + j, pl.ds(2 * p, 2)].reshape(2 * ROWS, kw)
                    v = jnp.dot(pmat[p], rows, preferred_element_type=f32).astype(bf16)
                    xg[:, pl.ds(p * 16, 16), j * kw:(j + 1) * kw] = v.reshape(n_exp, 16, kw)
            return carry

        lax.fori_loop(0, 4, gather, 0)

        def experts(g, carry):
            for copy in w_copies(s, g):
                copy.wait()
            for u in range(GRP):
                e = g * GRP + u
                xe = xg[e, :, 0:width]
                a = proj(wgs[g, u, :, 0:width], xe)
                b = proj(wus[g, u, :, 0:width], xe)
                if s > 0:
                    a = acc_a[e] + a
                    b = acc_b[e] + b
                if s < len(STEPS) - 1:
                    acc_a[e] = a
                    acc_b[e] = b
                else:
                    h = jax.nn.silu(a) * b
                    hbuf[e] = (h.T if FLIP else h).astype(bf16)
            if s < len(STEPS) - 1:
                for copy in w_copies(s + 1, g):
                    copy.start()
            return carry

        if between:
            lax.fori_loop(0, n_grp // 2, experts, 0)
            between[0]()
            lax.fori_loop(n_grp // 2, n_grp, experts, 0)
        else:
            lax.fori_loop(0, n_grp, experts, 0)
        for step in between[1:]:
            step()

    def chunks(step, *ks):
        def run():
            for k in ks:
                step(k)
        return run

    for k in (1, 2): step_a(k)
    step_b(0)
    wait_sibling(0)
    compute(0, chunks(step_a, 3), chunks(step_b, 1))
    step_a(4)
    step_b(2)
    chunks(wait_sibling, 1, 2)()
    compute(1, chunks(step_a, 5), chunks(step_b, 3))
    step_a(6)
    step_b(4)
    chunks(wait_sibling, 3, 4)()
    compute(2, chunks(step_a, 7), chunks(step_b, 5))
    step_b(6)
    chunks(wait_sibling, 5, 6)()
    compute(3, chunks(step_b, 7))
    wait_sibling(7)
    compute(4)

    def down(n):
        def body(g, carry):
            wd_copy(n, g).wait()
            for u in range(GRP):
                e = g * GRP + u
                o = jnp.dot(hbuf[e], wds[n % 2, e, :, 0:WIDTHS[n]], preferred_element_type=f32)
                gt = gbuf[e]
                o = o * jnp.concatenate([gt] * (WIDTHS[n] // 128), axis=1)
                parts = []
                for i in range(3):
                    part = o.astype(bf16)
                    if i < 2:
                        o = o - part.astype(f32)
                    parts.append(part)
                for i in range(3):
                    obuf[:, i, e, :, 0:WIDTHS[n]] = parts[i].reshape(8, 16, WIDTHS[n])
            return carry

        lax.fori_loop(0, n_grp, body, 0)
        if n + 2 < nc:
            for g in range(n_grp):
                wd_copy(n + 2, g).start()

    def merged(n, p):
        v = jnp.dot(cmat[p], obuf[p, :, :, :, 0:WIDTHS[n]].reshape(768, WIDTHS[n]), preferred_element_type=f32)
        return v.reshape(2, ROWS, WIDTHS[n])

    def cols(n):
        return pl.ds(0, WIDTHS[n])

    def part(ref, n, slot, q):
        return ref.at[slot, pl.ds(2 * (q % 2), 2), q // 2, :, cols(n)]

    sib_sends = {}

    def combine(n):
        if n >= 2:
            for copy in sib_sends.pop(n - 2):
                copy.wait_send()
        out = []
        for q in range(4):
            part(psib, n, n % 2, q)[...] = merged(n, (1 - c) * 4 + q)
        for q in range(4):
            copy = rcopy(part(psib, n, n % 2, q), part(rd, n, n, q), ds_s.at[n, q], ds_r.at[n, q], sib)
            copy.start()
            out.append(copy)
        sib_sends[n] = out
        for q in range(4):
            part(pown, n, n, q)[...] = merged(n, c * 4 + q)

    def add(dst, src):
        dst[...] = dst[...] + src[...]

    def core_total(n):
        for q in range(4):
            buf = part(rd, n, n, q)
            rcopy(buf, buf, ds_s.at[n, q], ds_r.at[n, q], sib).wait_recv()
            add(part(pown, n, n, q), buf)

    def piece(n, d):
        return pown.at[n, d] if n in ZFIRST else pown.at[n, d, y, :, cols(n)]

    def r_buf(n, d):
        return rr2.at[ZFIRST.index(n), d] if n in ZFIRST else rr.at[n, d, :, cols(n)]

    def l_buf(n, d):
        return rl2.at[ZFIRST.index(n), d] if n in ZFIRST else rl.at[n, d, :, cols(n)]

    def hop(n, at, right):
        buf, ssem, rsem = (r_buf, rr_s, rr_r) if right else (l_buf, rl_s, rl_r)
        dests = range(3, at, -1) if right else range(0, at)
        here = z == at

        def onward(n, d):
            return rcopy(piece(n, d), buf(n, d), ssem.at[n, d], rsem.at[n, d],
                         {"tp": (z + (1 if right else 3)) % 4})

        @pl.when(here)
        def _():
            for d in dests:
                if 0 < at < 3:
                    rcopy(buf(n, d), buf(n, d), ssem.at[n, d], rsem.at[n, d], sib).wait_recv()
                    add(piece(n, d), buf(n, d))
                onward(n, d).start()

        hops.append((here, [functools.partial(onward, n, d) for d in dests]))

    def z_total(n):
        @pl.when(z > 0)
        def _():
            rcopy(r_buf(n, z), r_buf(n, z), rr_s.at[n, z], rr_r.at[n, z], sib).wait_recv()
            add(piece(n, z), r_buf(n, z))

        @pl.when(z < 3)
        def _():
            rcopy(l_buf(n, z), l_buf(n, z), rl_s.at[n, z], rl_r.at[n, z], sib).wait_recv()
            add(piece(n, z), l_buf(n, z))

    def y_buf(n):
        return ry.at[n, pl.ds(0, 1)] if n in ZFIRST else ry.at[n, :, :, cols(n)]

    def y_send(n):
        src = pown.at[n, pl.ds(z, 1), 1 - y] if n in ZFIRST else pown.at[n, :, 1 - y, :, cols(n)]
        send(src, y_buf(n), ys_s.at[n], ys_r.at[n], yn)

    def y_add(n):
        rcopy(y_buf(n), y_buf(n), ys_s.at[n], ys_r.at[n], sib).wait_recv()
        add(pown.at[n, pl.ds(z, 1), y] if n in ZFIRST else pown.at[n, :, y, :, cols(n)], y_buf(n))

    def finish(n):
        out_ref[:, starts[n]:starts[n] + WIDTHS[n]] = pown[n, z, y, :, 0:WIDTHS[n]].astype(bf16)

    def y_hop(n):
        y_add(n)
        hop(n, 0, True)
        hop(n, 3, False)

    def hop_1(n):
        hop(n, 1, True)
        hop(n, 2, False)

    def hop_2(n):
        hop(n, 2, True)
        hop(n, 1, False)

    def straight(n, i):
        d = (z + i) % 4
        return rcopy(piece(n, d), rr.at[n, z, :, cols(n)], rr_s.at[n, i], rr_r.at[n, z], {"tp": d})

    def y_straight(n):
        y_add(n)
        for i in (2, 1, 3):
            copy = straight(n, i)
            copy.start()
            sends.append(copy)

    def straight_end(n):
        for i in (1, 3, 2):
            buf = r_buf(n, (z + i) % 4)
            rcopy(buf, buf, rr_s.at[n, i], rr_r.at[n, (z + i) % 4], sib).wait_recv()
            add(piece(n, z), buf)
        finish(n)

    def z_end(n):
        z_total(n)
        if n in ZFIRST:
            y_send(n)
        else:
            finish(n)

    def y_end(n):
        y_add(n)
        finish(n)

    def first(n):
        core_total(n)
        if n in ZFIRST:
            hop(n, 0, True)
            hop(n, 3, False)
        else:
            y_send(n)

    plan = {n: {2: y_hop, 3: hop_1, 4: hop_2, 5: z_end} for n in range(nc)}
    plan.update({n: {2: hop_1, 3: hop_2, 4: z_end, 6: y_end} for n in ZFIRST})
    plan.update({n: {2: y_straight, 3: straight_end} for n in DIRECT})
    for t in range(nc + 6):
        if t < nc:
            down(t)
            combine(t)
        for lag in range(6, 0, -1):
            n = t - lag
            if 0 <= n < nc and lag in plan[n]:
                plan[n][lag](n)
        if t < nc:
            first(t)

    for out in sib_sends.values():
        for copy in out:
            copy.wait_send()
    for copy in sends:
        copy.wait_send()
    for here, makers in hops:
        @pl.when(here)
        def _():
            for maker in makers:
                maker().wait_send()


def solution(mesh):
    row_spec = P(("dp", "ep", "tp"), None)

    def local_moe(x, ids, gates, wg, wu, wd):
        rows, d_model = x.shape
        n_exp, _, ff = wg.shape
        nc = len(WIDTHS)
        kw = d_model // NK
        f32, bf16 = jnp.float32, jnp.bfloat16
        vm, dma = pltpu.VMEM, pltpu.SemaphoreType.DMA
        whole = pl.BlockSpec(memory_space=pltpu.VMEM)
        far = pl.BlockSpec(memory_space=pl.ANY)
        return pl.pallas_call(
            moe_kernel,
            out_shape=jax.ShapeDtypeStruct((rows, d_model), bf16),
            in_specs=[whole, whole, whole, far, far, far],
            out_specs=whole,
            scratch_shapes=[
                vm((NK, 16, rows, kw), bf16),
                vm((n_exp, 128, 2 * kw), bf16),
                vm((16, 16, 128), f32),
                vm((8, 256, 128), bf16),
                vm((8, 128, 768), bf16),
                vm((n_exp, 128, 128), f32),
                vm((n_exp, ff, 128) if FLIP else (n_exp, 128, ff), f32),
                vm((n_exp, ff, 128) if FLIP else (n_exp, 128, ff), f32),
                vm((n_exp, 128, ff), bf16),
                vm((8, 3, n_exp, 16, CW), bf16),
                vm((n_exp // GRP, GRP, ff, 2 * kw), bf16),
                vm((n_exp // GRP, GRP, ff, 2 * kw), bf16),
                vm((2, n_exp, ff, CW), bf16),
                vm((nc, 4, 2, rows, CW), f32),
                vm((2, 4, 2, rows, CW), f32),
                vm((nc, 4, 2, rows, CW), f32),
                vm((nc, 4, rows, CW), f32),
                vm((nc, 4, rows, CW), f32),
                vm((len(ZFIRST), 4, 2, rows, CW), f32),
                vm((len(ZFIRST), 4, 2, rows, CW), f32),
                vm((nc, 4, rows, CW), f32),
                dma((NK, 16)), dma((NK, 16)), dma((15,)), dma((16,)),
                dma((2, n_exp // GRP)), dma((2, n_exp // GRP)),
                dma((nc, 4)), dma((nc, 4)), dma((nc, 4)), dma((nc, 4)),
                dma((nc, 4)), dma((nc, 4)), dma((nc,)), dma((nc,)),
            ],
            compiler_params=pltpu.CompilerParams(
                collective_id=0, has_side_effects=True, vmem_limit_bytes=66_000_000),
        )(x, ids.T, gates.T, wg.swapaxes(1, 2), wu.swapaxes(1, 2), wd)

    return jax.shard_map(
        local_moe, mesh=mesh,
        in_specs=(row_spec, row_spec, row_spec, P("ep", None, "tp"), P("ep", None, "tp"), P("ep", "tp", None)),
        out_specs=row_spec, check_vma=False)
```

```python
import functools

import jax
import jax.numpy as jnp
from jax import lax
from jax.experimental import pallas as pl
from jax.experimental.pallas import tpu as pltpu
from jax.sharding import PartitionSpec as P

MESH = pl.DeviceIdType.MESH
NK = 8
STEPS = ((0, 1), (1, 2), (3, 2), (5, 2), (7, 1))
CW = 256
WIDTHS = (256,) * 8
GRP = 8
SLOTS = 8
ROWS = 64
TOPK = 6
AHEAD = 3
FLIP = True
DIRECT = (7,)
ZFIRST = (1,)


def moe_kernel(x_hbm, ids_hbm, gate_hbm, wg, wu, wd, out_hbm,
               x_ref, ids_ref, gate_ref, out_ref, in_sem, out_sem, xall, xg, meta, pmat, cmat, gbuf, acc_a, acc_b, hbuf, obuf,
               wgs, wus, wds, pown, psib, rd, rr, rl, rr2, rl2, ry,
               ags, agr, mss, msr, wsem, wdsem,
               ds_s, ds_r, rr_s, rr_r, rl_s, rl_r, ys_s, ys_r):
    f32, bf16 = jnp.float32, jnp.bfloat16
    d_model = x_ref.shape[1]
    kw = d_model // NK
    nc = len(WIDTHS)
    starts = [sum(WIDTHS[:n]) for n in range(nc)]
    n_exp = wg.shape[0]
    n_grp = n_exp // GRP

    z = lax.axis_index("tp")
    ep = lax.axis_index("ep")
    y = ep // 2
    c = ep % 2
    sib = {"ep": 2 * y + 1 - c}
    yn = {"ep": 2 * (1 - y) + c}
    sends = []
    hops = []

    def rcopy(src, dst, ssem, rsem, dev):
        return pltpu.make_async_remote_copy(src_ref=src, dst_ref=dst, send_sem=ssem, recv_sem=rsem,
                                            device_id=dev, device_id_type=MESH)

    def send(*args):
        copy = rcopy(*args)
        copy.start()
        sends.append(copy)

    def w_copies(s, g):
        rows = pl.ds(g * GRP, GRP)
        cols = pl.ds(STEPS[s][0] * kw, STEPS[s][1] * kw)
        here = pl.ds(0, STEPS[s][1] * kw)
        return (pltpu.make_async_copy(wg.at[rows, :, cols], wgs.at[g, :, :, here], wsem.at[0, g]),
                pltpu.make_async_copy(wu.at[rows, :, cols], wus.at[g, :, :, here], wsem.at[1, g]))

    def wd_copy(n, g):
        rows = pl.ds(g * GRP, GRP)
        return pltpu.make_async_copy(wd.at[rows, :, pl.ds(starts[n], WIDTHS[n])],
                                     wds.at[n % 2, rows, :, pl.ds(0, WIDTHS[n])], wdsem.at[n % 2, g])

    loads = [pltpu.make_async_copy(src, dst, in_sem.at[i]) for i, (src, dst) in
             enumerate(((x_hbm, x_ref), (ids_hbm, ids_ref), (gate_hbm, gate_ref)))]
    for copy in loads:
        copy.start()
    for g in range(n_grp):
        for copy in w_copies(0, g):
            copy.start()
    for n in range(2):
        for g in range(n_grp):
            wd_copy(n, g).start()

    barrier = pltpu.get_barrier_semaphore()
    peers = [{"ep": (ep + d // 4) % 4, "tp": (z + d % 4) % 4} for d in range(1, 16)]
    for peer in peers:
        pl.semaphore_signal(barrier, inc=1, device_id=peer, device_id_type=MESH)
    for copy in loads:
        copy.wait()
    pl.semaphore_wait(barrier, 15)

    def idx(cc, yy, zz):
        return cc * 8 + yy * 4 + zz

    me = idx(c, y, z)

    def send_block(k, slot, b, dev):
        src = x_ref.at[:, pl.ds(k * kw, kw)] if b is me else xall.at[k, b]
        send(src, xall.at[k, b], ags.at[k, slot], agr.at[k, b], dev)

    def wait_block(k, b):
        rcopy(xall.at[k, b], xall.at[k, b], ags.at[k, 0], agr.at[k, b], sib).wait_recv()

    def z_block(k, i):
        return rcopy(x_ref.at[:, pl.ds(k * kw, kw)], xall.at[k, me], ags.at[k, i], agr.at[k, me],
                     {"tp": (z + i) % 4})

    def relay(k):
        b = idx(c, y, 3 * (2 - z))
        return rcopy(xall.at[k, b], xall.at[k, b], ags.at[k, 15], agr.at[k, b], {"tp": 3 * (z - 1)})

    inner = (z == 1) | (z == 2)
    near = {1: z < 3, 2: None, 3: z > 0}

    def send_z(k):
        for i in (2, 1, 3):
            if near[i] is None:
                copy = z_block(k, i)
                copy.start()
                sends.append(copy)
            else:
                pl.when(near[i])(lambda: z_block(k, i).start())
                hops.append((near[i], [functools.partial(z_block, k, i)]))

    def send_own(k):
        send_block(k, 0, me, yn)
        send_block(k, 4, me, sib)

    def step_a(k):
        for i in (2, 1, 3):
            b = idx(c, y, (z + i) % 4)
            wait_block(k, b)
            if i == 2:
                pl.when(inner)(lambda: relay(k).start())
                hops.append((inner, [functools.partial(relay, k)]))
                if k + AHEAD < NK:
                    send_z(k + AHEAD)
            send_block(k, 4 + i, b, yn)
            send_block(k, 7 + i, b, sib)

    def step_b(k):
        for i in range(4):
            b = idx(c, 1 - y, (z + i) % 4)
            wait_block(k, b)
            send_block(k, 11 + i, b, sib)

    def wait_sibling(k):
        for b in range(8):
            wait_block(k, (1 - c) * 8 + b)

    send_z(0)
    send_own(0)

    lane = lax.broadcasted_iota(jnp.int32, (128, 128), 1)
    sub = lax.broadcasted_iota(jnp.int32, (128, 128), 0)
    tri = jnp.where((sub < lane % ROWS) & (sub < ROWS), 1.0, 0.0).astype(bf16)

    def twice(v):
        v = jnp.concatenate([v, v], axis=1)
        return jnp.concatenate([v, jnp.zeros((8 - TOPK, 128), f32)], axis=0)

    ids_t = twice(ids_ref[...].astype(f32))
    gate_t = twice(gate_ref[...])
    exp_id = lax.broadcasted_iota(jnp.int32, (64, 128), 0).astype(f32)
    hits = [jnp.where(exp_id == ids_t[j:j + 1], 1.0, 0.0) for j in range(TOPK)]
    chosen = functools.reduce(lambda p, q: p + q, hits)
    rank = jnp.dot(chosen.astype(bf16), tri, preferred_element_type=f32)
    code = [SLOTS * ids_t[j:j + 1] + jnp.sum(rank * hits[j], axis=0, keepdims=True) for j in range(TOPK)]
    code = jnp.concatenate(code + [jnp.full((8 - TOPK, 128), -1.0, f32)], axis=0)
    meta[me, 0:8, :] = code
    meta[me, 8:16, :] = gate_t
    for k in range(NK):
        xall[k, me] = x_ref[:, k * kw:(k + 1) * kw]
    for d, peer in enumerate(peers):
        send(meta.at[me], meta.at[me], mss.at[d], msr.at[me], peer)
    for k in range(1, NK):
        if k < AHEAD:
            send_z(k)
        send_own(k)

    step_a(0)

    for d in range(1, 16):
        s_ep, s_z = (ep + d // 4) % 4, (z + d % 4) % 4
        b = idx(s_ep % 2, s_ep // 2, s_z)
        rcopy(meta.at[b], meta.at[b], mss.at[0], msr.at[b], sib).wait_recv()

    def build(p, carry):
        half = lax.broadcasted_iota(jnp.int32, (8, 128), 1) < ROWS
        both = jnp.where(half, meta[2 * p, 0:8, :], meta[2 * p + 1, 0:8, :]).astype(jnp.int32)
        gts = jnp.where(half, meta[2 * p, 8:16, :], meta[2 * p + 1, 8:16, :])
        expert = lax.shift_right_arithmetic(both, 3)
        slot = both - expert * SLOTS
        row = (expert - ep * n_exp) * (2 * SLOTS) + jnp.where(half, 0, SLOTS) + slot
        r = lax.broadcasted_iota(jnp.int32, (n_exp * 2 * SLOTS, 128), 0)
        sel = jnp.zeros(r.shape, f32)
        wts = jnp.zeros(r.shape, f32)
        for j in range(TOPK):
            eq = r == row[j:j + 1]
            sel = jnp.where(eq, 1.0, sel)
            wts = jnp.where(eq, gts[j:j + 1], wts)
        pmat[p] = sel.astype(bf16)
        selt = sel.T.astype(bf16)
        cmat[p] = jnp.concatenate([selt, selt, selt], axis=1)
        per_row = jnp.broadcast_to(jnp.sum(wts, axis=1, keepdims=True), wts.shape)
        gbuf[:, pl.ds(p * 16, 16), :] = per_row.reshape(n_exp, 16, 128)
        return carry

    lax.fori_loop(0, 8, build, 0)

    def proj(w, xe):
        dims = (((1,), (1,)), ((), ()))
        if FLIP:
            return lax.dot_general(w, xe, dims, preferred_element_type=f32)
        return lax.dot_general(xe, w, dims, preferred_element_type=f32)

    def compute(s, *between):
        k0, count = STEPS[s]
        width = count * kw

        def gather(i, carry):
            for u in range(2):
                p = i * 2 + u
                for j in range(count):
                    rows = xall[k0 + j, pl.ds(2 * p, 2)].reshape(2 * ROWS, kw)
                    v = jnp.dot(pmat[p], rows, preferred_element_type=f32).astype(bf16)
                    xg[:, pl.ds(p * 16, 16), j * kw:(j + 1) * kw] = v.reshape(n_exp, 16, kw)
            return carry

        lax.fori_loop(0, 4, gather, 0)

        def experts(g, carry):
            for copy in w_copies(s, g):
                copy.wait()
            for u in range(GRP):
                e = g * GRP + u
                xe = xg[e, :, 0:width]
                a = proj(wgs[g, u, :, 0:width], xe)
                b = proj(wus[g, u, :, 0:width], xe)
                if s > 0:
                    a = acc_a[e] + a
                    b = acc_b[e] + b
                if s < len(STEPS) - 1:
                    acc_a[e] = a
                    acc_b[e] = b
                else:
                    h = jax.nn.silu(a) * b
                    hbuf[e] = (h.T if FLIP else h).astype(bf16)
            if s < len(STEPS) - 1:
                for copy in w_copies(s + 1, g):
                    copy.start()
            return carry

        if between:
            lax.fori_loop(0, n_grp // 2, experts, 0)
            between[0]()
            lax.fori_loop(n_grp // 2, n_grp, experts, 0)
        else:
            lax.fori_loop(0, n_grp, experts, 0)
        for step in between[1:]:
            step()

    def chunks(step, *ks):
        def run():
            for k in ks:
                step(k)
        return run

    for k in (1, 2): step_a(k)
    step_b(0)
    wait_sibling(0)
    compute(0, chunks(step_a, 3), chunks(step_b, 1))
    step_a(4)
    step_b(2)
    chunks(wait_sibling, 1, 2)()
    compute(1, chunks(step_a, 5), chunks(step_b, 3))
    step_a(6)
    step_b(4)
    chunks(wait_sibling, 3, 4)()
    compute(2, chunks(step_a, 7), chunks(step_b, 5))
    step_b(6)
    chunks(wait_sibling, 5, 6)()
    compute(3, chunks(step_b, 7))
    wait_sibling(7)
    compute(4)

    def down(n):
        def body(g, carry):
            wd_copy(n, g).wait()
            for u in range(GRP):
                e = g * GRP + u
                o = jnp.dot(hbuf[e], wds[n % 2, e, :, 0:WIDTHS[n]], preferred_element_type=f32)
                gt = gbuf[e]
                o = o * jnp.concatenate([gt] * (WIDTHS[n] // 128), axis=1)
                parts = []
                for i in range(3):
                    part = o.astype(bf16)
                    if i < 2:
                        o = o - part.astype(f32)
                    parts.append(part)
                for i in range(3):
                    obuf[:, i, e, :, 0:WIDTHS[n]] = parts[i].reshape(8, 16, WIDTHS[n])
            return carry

        lax.fori_loop(0, n_grp, body, 0)
        if n + 2 < nc:
            for g in range(n_grp):
                wd_copy(n + 2, g).start()

    def merged(n, p):
        v = jnp.dot(cmat[p], obuf[p, :, :, :, 0:WIDTHS[n]].reshape(768, WIDTHS[n]), preferred_element_type=f32)
        return v.reshape(2, ROWS, WIDTHS[n])

    def cols(n):
        return pl.ds(0, WIDTHS[n])

    def part(ref, n, slot, q):
        return ref.at[slot, pl.ds(2 * (q % 2), 2), q // 2, :, cols(n)]

    sib_sends = {}

    def combine(n):
        if n >= 2:
            for copy in sib_sends.pop(n - 2):
                copy.wait_send()
        out = []
        for q in range(4):
            part(psib, n, n % 2, q)[...] = merged(n, (1 - c) * 4 + q)
        for q in range(4):
            copy = rcopy(part(psib, n, n % 2, q), part(rd, n, n, q), ds_s.at[n, q], ds_r.at[n, q], sib)
            copy.start()
            out.append(copy)
        sib_sends[n] = out
        for q in range(4):
            part(pown, n, n, q)[...] = merged(n, c * 4 + q)

    def add(dst, src):
        dst[...] = dst[...] + src[...]

    def core_total(n):
        for q in range(4):
            buf = part(rd, n, n, q)
            rcopy(buf, buf, ds_s.at[n, q], ds_r.at[n, q], sib).wait_recv()
            add(part(pown, n, n, q), buf)

    def piece(n, d):
        return pown.at[n, d] if n in ZFIRST else pown.at[n, d, y, :, cols(n)]

    def r_buf(n, d):
        return rr2.at[ZFIRST.index(n), d] if n in ZFIRST else rr.at[n, d, :, cols(n)]

    def l_buf(n, d):
        return rl2.at[ZFIRST.index(n), d] if n in ZFIRST else rl.at[n, d, :, cols(n)]

    def hop(n, at, right):
        buf, ssem, rsem = (r_buf, rr_s, rr_r) if right else (l_buf, rl_s, rl_r)
        dests = range(3, at, -1) if right else range(0, at)
        here = z == at

        def onward(n, d):
            return rcopy(piece(n, d), buf(n, d), ssem.at[n, d], rsem.at[n, d],
                         {"tp": (z + (1 if right else 3)) % 4})

        @pl.when(here)
        def _():
            for d in dests:
                if 0 < at < 3:
                    rcopy(buf(n, d), buf(n, d), ssem.at[n, d], rsem.at[n, d], sib).wait_recv()
                    add(piece(n, d), buf(n, d))
                onward(n, d).start()

        hops.append((here, [functools.partial(onward, n, d) for d in dests]))

    def z_total(n):
        @pl.when(z > 0)
        def _():
            rcopy(r_buf(n, z), r_buf(n, z), rr_s.at[n, z], rr_r.at[n, z], sib).wait_recv()
            add(piece(n, z), r_buf(n, z))

        @pl.when(z < 3)
        def _():
            rcopy(l_buf(n, z), l_buf(n, z), rl_s.at[n, z], rl_r.at[n, z], sib).wait_recv()
            add(piece(n, z), l_buf(n, z))

    def y_buf(n):
        return ry.at[n, pl.ds(0, 1)] if n in ZFIRST else ry.at[n, :, :, cols(n)]

    def y_send(n):
        src = pown.at[n, pl.ds(z, 1), 1 - y] if n in ZFIRST else pown.at[n, :, 1 - y, :, cols(n)]
        send(src, y_buf(n), ys_s.at[n], ys_r.at[n], yn)

    def y_add(n):
        rcopy(y_buf(n), y_buf(n), ys_s.at[n], ys_r.at[n], sib).wait_recv()
        add(pown.at[n, pl.ds(z, 1), y] if n in ZFIRST else pown.at[n, :, y, :, cols(n)], y_buf(n))

    def out_copy(n):
        span = pl.ds(starts[n], WIDTHS[n])
        return pltpu.make_async_copy(out_ref.at[:, span], out_hbm.at[:, span], out_sem.at[n])

    def finish(n):
        out_ref[:, starts[n]:starts[n] + WIDTHS[n]] = pown[n, z, y, :, 0:WIDTHS[n]].astype(bf16)
        out_copy(n).start()

    def y_hop(n):
        y_add(n)
        hop(n, 0, True)
        hop(n, 3, False)

    def hop_1(n):
        hop(n, 1, True)
        hop(n, 2, False)

    def hop_2(n):
        hop(n, 2, True)
        hop(n, 1, False)

    def straight(n, i):
        d = (z + i) % 4
        return rcopy(piece(n, d), rr.at[n, z, :, cols(n)], rr_s.at[n, i], rr_r.at[n, z], {"tp": d})

    def y_straight(n):
        y_add(n)
        for i in (2, 1, 3):
            copy = straight(n, i)
            copy.start()
            sends.append(copy)

    def straight_end(n):
        for i in (1, 3, 2):
            buf = r_buf(n, (z + i) % 4)
            rcopy(buf, buf, rr_s.at[n, i], rr_r.at[n, (z + i) % 4], sib).wait_recv()
            add(piece(n, z), buf)
        finish(n)

    def z_end(n):
        z_total(n)
        if n in ZFIRST:
            y_send(n)
        else:
            finish(n)

    def y_end(n):
        y_add(n)
        finish(n)

    def first(n):
        core_total(n)
        if n in ZFIRST:
            hop(n, 0, True)
            hop(n, 3, False)
        else:
            y_send(n)

    plan = {n: {2: y_hop, 3: hop_1, 4: hop_2, 5: z_end} for n in range(nc)}
    plan.update({n: {2: hop_1, 3: hop_2, 4: z_end, 6: y_end} for n in ZFIRST})
    plan.update({n: {2: y_straight, 3: straight_end} for n in DIRECT})
    for t in range(nc + 6):
        if t < nc:
            down(t)
            combine(t)
        for lag in range(6, 0, -1):
            n = t - lag
            if 0 <= n < nc and lag in plan[n]:
                plan[n][lag](n)
        if t < nc:
            first(t)

    for out in sib_sends.values():
        for copy in out:
            copy.wait_send()
    for copy in sends:
        copy.wait_send()
    for n in range(nc):
        out_copy(n).wait()
    for here, makers in hops:
        @pl.when(here)
        def _():
            for maker in makers:
                maker().wait_send()


def solution(mesh):
    row_spec = P(("dp", "ep", "tp"), None)

    def local_moe(x, ids, gates, wg, wu, wd):
        rows, d_model = x.shape
        n_exp, _, ff = wg.shape
        nc = len(WIDTHS)
        kw = d_model // NK
        f32, bf16 = jnp.float32, jnp.bfloat16
        vm, dma = pltpu.VMEM, pltpu.SemaphoreType.DMA
        far = pl.BlockSpec(memory_space=pl.ANY)
        return pl.pallas_call(
            moe_kernel,
            out_shape=jax.ShapeDtypeStruct((rows, d_model), bf16),
            in_specs=[far] * 6,
            out_specs=far,
            scratch_shapes=[
                vm((rows, d_model), bf16), vm((TOPK, rows), jnp.int32), vm((TOPK, rows), f32), vm((rows, d_model), bf16),
                dma((3,)), dma((nc,)),
                vm((NK, 16, rows, kw), bf16),
                vm((n_exp, 128, 2 * kw), bf16),
                vm((16, 16, 128), f32),
                vm((8, 256, 128), bf16),
                vm((8, 128, 768), bf16),
                vm((n_exp, 128, 128), f32),
                vm((n_exp, ff, 128) if FLIP else (n_exp, 128, ff), f32),
                vm((n_exp, ff, 128) if FLIP else (n_exp, 128, ff), f32),
                vm((n_exp, 128, ff), bf16),
                vm((8, 3, n_exp, 16, CW), bf16),
                vm((n_exp // GRP, GRP, ff, 2 * kw), bf16),
                vm((n_exp // GRP, GRP, ff, 2 * kw), bf16),
                vm((2, n_exp, ff, CW), bf16),
                vm((nc, 4, 2, rows, CW), f32),
                vm((2, 4, 2, rows, CW), f32),
                vm((nc, 4, 2, rows, CW), f32),
                vm((nc, 4, rows, CW), f32),
                vm((nc, 4, rows, CW), f32),
                vm((len(ZFIRST), 4, 2, rows, CW), f32),
                vm((len(ZFIRST), 4, 2, rows, CW), f32),
                vm((nc, 4, rows, CW), f32),
                dma((NK, 16)), dma((NK, 16)), dma((15,)), dma((16,)),
                dma((2, n_exp // GRP)), dma((2, n_exp // GRP)),
                dma((nc, 4)), dma((nc, 4)), dma((nc, 4)), dma((nc, 4)),
                dma((nc, 4)), dma((nc, 4)), dma((nc,)), dma((nc,)),
            ],
            compiler_params=pltpu.CompilerParams(
                collective_id=0, has_side_effects=True, vmem_limit_bytes=66_000_000),
        )(x, ids.T, gates.T, wg.swapaxes(1, 2), wu.swapaxes(1, 2), wd)

    return jax.shard_map(
        local_moe, mesh=mesh,
        in_specs=(row_spec, row_spec, row_spec, P("ep", None, "tp"), P("ep", None, "tp"), P("ep", "tp", None)),
        out_specs=row_spec, check_vma=False)
```
